32 devices in a mesh: lat: 8 (over z, x), lon: 4 (over y, core).
Axes of the slice: x: 2, y: 2, z: 4, core: 2. Of those that a mesh axis runs over, the one named last changes fastest.
Arguments:
- courant: float32 [2, 16, 128, 512], P(None, None, 'lat', 'lon'), may hold values from -0.45 to 0.45
- obs_matrix: float32 [8, 32, 128, 128], P('lat', 'lon'), may hold values from -0.5 to 0.5
- obs_weight: float32 [8, 32, 128], P('lat', 'lon'), may hold values from 0.5 to 4
- innovation: float32 [8, 32, 128], P('lat', 'lon'), may hold values from -6 to 6
- block_owner: int32 [8, 32, 1], P('lat', 'lon'), may hold values from 0 to 3; in each aligned block of 8 rows (0 to 7, 8 to 15, ..., all dimensions but the last counted through in order) at most 2 rows name the same one
- block_row: int32 [8, 32], P('lat', 'lon'), may hold values from 0 to 255
- block_count: int32 [8, 4], P('lat', 'lon'), may hold values from 1 to 8, as said below
Outputs:
- increment: float32 [16, 128, 512], P(None, 'lat', 'lon')
- residual: float32 [16, 128, 512], P(None, 'lat', 'lon')
The draws below stay inside these ranges and needn't reach their ends.
Inputs may be any that keep to these rules, and one draw needn't show every extreme that they name: `block_owner`: among one device's 8 block slots no lon index is named more than 2 times, a bound that some block reaches. A device's first block_count slots are live, the rest are padding; some device has all 8 live.
All inputs are finite; a program needn't handle non-finite values.
Results may differ from the reference program's by a relative error of at most 0.0003.
Values sent between devices are 32-bit elements; how exact they have to be, the bound alone decides.
A program may use at most 64 MiB of HBM per device.

```python
import math
import jax
import jax.numpy as jnp
import numpy as np
from jax import lax

LEVELS = 16
CLAT = 16
CLON = 128
OBS = 128
CAP = 8
SLOT = 2
STEPS = 4
ITERS = 2
NLAT = 128
NLON = 512
BLOCKS = 32
N_LAT = 8
N_LON = 4


def draw_block_count(key, part):
    first_key, second_key = jax.random.split(jax.random.fold_in(key, 11))
    counted = jax.random.randint(first_key, (N_LAT * N_LON,), 1, CAP + 1)
    chosen = jax.random.randint(second_key, (), 0, N_LAT * N_LON)
    counted = jnp.where(jnp.arange(N_LAT * N_LON) == chosen, CAP, counted)
    return counted.reshape(N_LAT, N_LON).astype(jnp.int32)


def place_ends(drawn, key, smallest, high):
    dims = drawn.shape
    place = [jax.random.randint(jax.random.fold_in(key, axis), (), 0, dims[axis]) for axis in range(len(dims))]
    drawn = drawn.at[tuple(place)].set(smallest)
    longest = dims.index(max(dims))
    place[longest] = (place[longest] + 1) % dims[longest]
    return drawn.at[tuple(place)].set(high)


def block_scale(own_key, dims, cuts, smallest, high):
    def one(position, blocks):
        draws = jax.random.uniform(jax.random.fold_in(jax.random.fold_in(own_key, 6), position), (blocks,), jnp.float32, smallest / len(cuts), high / len(cuts))
        return jnp.repeat(jnp.exp(draws), dims[position] // blocks).reshape((-1,) + (1,) * (len(dims) - position - 1))

    level = one(*cuts[0])
    for cut in cuts[1:]:
        level = level * one(*cut)
    return level


def routed_block(rng, own, number, rows, number_of, top, reach, slope):
    sequence = jax.random.permutation(rng, number_of)
    heavy_load, usual = portions_of(number_of, rows * top, reach, slope, True), portions_of(number_of, rows * top, reach, slope, False)
    places = jnp.arange(number_of)

    def named(lengths, offset_by):
        used = int((lengths > 0).sum())
        fixed = max(1, used // 4)
        moved = fixed + (places - fixed + offset_by * (used - fixed)) % max(1, number_of - fixed)
        return jnp.zeros((number_of,), jnp.int32).at[sequence[jnp.where(places < fixed, places, moved)]].set(jnp.asarray(lengths, jnp.int32))

    lengths = jnp.where(number % 4 == 0, named(heavy_load, number // 4), named(usual, number - number // 4 - 1))
    mixed = jax.random.permutation(jax.random.fold_in(own, 3), number_of)
    donor, sink = mixed[0:number_of // 2 * 2:2], mixed[1:number_of // 2 * 2:2]
    room = jnp.minimum(lengths[donor] - 1, reach - lengths[sink]) // 2
    room = jnp.where((donor == sequence[0]) | (sink == sequence[0]) | (lengths[sink] == 0), 0, jnp.maximum(room, 0))
    moved = jax.random.randint(jax.random.fold_in(own, 4), (number_of // 2,), 0, 1 << 20) % (room + 1)
    lengths = lengths.at[donor].add(-moved).at[sink].add(moved)
    items = jnp.searchsorted(jnp.cumsum(lengths), jnp.arange(rows * top), side="right").astype(jnp.int32)
    listing = items.reshape(top, rows).T
    listing = listing[jax.random.permutation(jax.random.fold_in(own, 1), rows)]
    offset_by = jax.random.randint(jax.random.fold_in(own, 2), (rows, 1), 0, top)
    return jnp.take_along_axis(listing, (jnp.arange(top)[None, :] + offset_by) % top, axis=1)


def portions_of(number_of, total, limit, slope, full):
    weights = [(1 << 20) // math.isqrt(rank ** slope) + 1 for rank in range(1, number_of + 1)]
    largest = limit if full else min(limit, max(-(-total // number_of), total * weights[0] // sum(weights)))
    least = 1 if total - largest >= number_of - 1 else 0
    given, spare = [largest] + [least] * (number_of - 1), total - largest - least * (number_of - 1)
    while spare > 0:
        movable = [i for i in range(1, number_of) if given[i] < largest] or [i for i in range(1, number_of) if given[i] < limit]
        pool, remaining = sum([weights[i] for i in movable]), spare
        for i in movable:
            addition = min(limit - given[i], max(1, remaining * weights[i] // pool), spare)
            given[i] = given[i] + addition
            spare = spare - addition
    return np.array(given)


def scatter_about(rng, extent, scale, limit, cuts=(), kind=jnp.bfloat16):
    level = block_scale(rng, extent, cuts, -0.22, 0.18) if cuts else 1.0
    array = jax.random.normal(rng, extent, jnp.float32) * scale * level
    return jnp.minimum(jnp.maximum(array, -limit), limit).astype(kind)


def setup_inputs(seed: int = 0) -> dict:
    splits = jax.random.split(jax.random.key(seed), 8)
    courant = jnp.clip(jax.random.uniform(splits[0], (2, LEVELS, NLAT, NLON), jnp.float32, -0.45, 0.45) * block_scale(splits[0], (2, LEVELS, NLAT, NLON), ((2, 8), (3, 4)), -0.4, 0.0), -0.45, 0.45)
    obs_matrix = scatter_about(splits[1], (N_LAT, BLOCKS, OBS, CLON), CLON ** -0.5, 0.5, ((0, 8), (1, 4)), jnp.float32)
    obs_weight = jnp.clip(jnp.exp(math.log(4.0) - 2.0794415 * jax.random.uniform(splits[2], (N_LAT, BLOCKS, OBS), jnp.float32) ** block_scale(splits[2], (N_LAT, BLOCKS, OBS), ((0, 8), (1, 4)), -0.2, 0.2)), 0.5, 4.0)
    innovation = scatter_about(splits[3], (N_LAT, BLOCKS, OBS), 1.0, 6.0, ((0, 8), (1, 4)), jnp.float32)
    block_owner_keys = jax.random.split(jax.random.fold_in(splits[4], 1), N_LAT * BLOCKS // CAP)
    block_owner_turns = jax.random.permutation(jax.random.fold_in(splits[4], 3), N_LAT * BLOCKS // CAP)
    block_owner = jax.vmap(lambda own, number: routed_block(jax.random.fold_in(splits[4], 2), own, number, CAP, N_LON, 1, SLOT, 2))(block_owner_keys, block_owner_turns).reshape((N_LAT, BLOCKS, 1))
    block_row = place_ends(jax.random.randint(splits[5], (N_LAT, BLOCKS), 0, LEVELS * CLAT), jax.random.fold_in(splits[5], 1), 0, (LEVELS * CLAT) - 1).astype(jnp.int32)
    block_count = draw_block_count(jax.random.fold_in(splits[7], 71), 0)
    return dict(courant=courant, obs_matrix=obs_matrix, obs_weight=obs_weight, innovation=innovation, block_owner=block_owner, block_row=block_row, block_count=block_count)


def from_south(grid_field):
    return jnp.pad(grid_field[:, :-1, :], ((0, 0), (1, 0), (0, 0)))


def from_north(grid_field):
    return jnp.pad(grid_field[:, 1:, :], ((0, 0), (0, 1), (0, 0)))


def tangent_step(grid_field, rate_parts, keep_self):
    return (keep_self * grid_field + rate_parts[0] * from_south(grid_field) + rate_parts[1] * from_north(grid_field)
            + rate_parts[2] * jnp.roll(grid_field, 1, axis=2) + rate_parts[3] * jnp.roll(grid_field, -1, axis=2))


def adjoint_step(grid_field, rate_parts, keep_self):
    return (keep_self * grid_field + from_north(rate_parts[0] * grid_field) + from_south(rate_parts[1] * grid_field)
            + jnp.roll(rate_parts[2] * grid_field, -1, axis=2) + jnp.roll(rate_parts[3] * grid_field, 1, axis=2))


def reference(courant, obs_matrix, obs_weight, innovation, block_owner, block_row, block_count):
    rate_parts = (jnp.maximum(courant[0], 0.0), jnp.maximum(-courant[0], 0.0),
                  jnp.maximum(courant[1], 0.0), jnp.maximum(-courant[1], 0.0))
    keep_self = 1.0 - rate_parts[0] - rate_parts[1] - rate_parts[2] - rate_parts[3]
    owner_lon = block_owner[:, :, 0]
    level_idx = block_row // CLAT
    lat_idx = jnp.arange(N_LAT, dtype=jnp.int32)[:, None] * CLAT + block_row % CLAT
    lon_idx = owner_lon[:, :, None] * CLON + jnp.arange(CLON, dtype=jnp.int32)[None, None, :]
    cell_index = ((level_idx * NLAT + lat_idx) * NLON)[:, :, None] + lon_idx
    slot_index = jnp.arange(BLOCKS, dtype=jnp.int32) % CAP
    live_mask = slot_index[None, :] < jnp.repeat(block_count, CAP, axis=1)
    weighted = jnp.where(live_mask[:, :, None], obs_weight, 0.0)

    def observe(grid_field):
        seen_rows = grid_field.reshape(-1)[cell_index]
        return jnp.einsum("ibok,ibk->ibo", obs_matrix, seen_rows, precision=lax.Precision.HIGHEST)

    def observe_adjoint(block_terms):
        spread = jnp.einsum("ibok,ibo->ibk", obs_matrix, block_terms, precision=lax.Precision.HIGHEST)
        flat_out = jnp.zeros((LEVELS * NLAT * NLON,), jnp.float32).at[cell_index].add(spread)
        return flat_out.reshape(LEVELS, NLAT, NLON)

    def model_adjoint(grid_field):
        for sweep in range(STEPS):
            grid_field = adjoint_step(grid_field, rate_parts, keep_self)
        return grid_field

    def hessian(vector):
        moved = vector
        for sweep in range(STEPS):
            moved = tangent_step(moved, rate_parts, keep_self)
        return vector + model_adjoint(observe_adjoint(weighted * observe(moved)))

    right_side = model_adjoint(observe_adjoint(weighted * innovation))
    increment = jnp.zeros_like(right_side)
    residual = right_side
    direction = right_side
    norm_now = jnp.sum(residual * residual)
    for sweep in range(ITERS):
        image_vec = hessian(direction)
        step_size = norm_now / jnp.sum(direction * image_vec)
        increment = increment + step_size * direction
        residual = residual - step_size * image_vec
        if sweep + 1 < ITERS:
            norm_next = jnp.sum(residual * residual)
            direction = residual + (norm_next / norm_now) * direction
            norm_now = norm_next
    return increment, residual
```

```python
import functools

import jax
import jax.numpy as jnp
from jax import lax
from jax.experimental import pallas as pl
from jax.experimental.pallas import tpu as pltpu
from jax.sharding import PartitionSpec as P

STEPS = 4
HALO = 2 * STEPS
MESH = pl.DeviceIdType.MESH
F32 = jnp.float32
BF16 = jnp.bfloat16


def split3(x):
    hi = x.astype(BF16)
    rest = x - hi.astype(F32)
    mid = rest.astype(BF16)
    low = (rest - mid.astype(F32)).astype(BF16)
    return hi, mid, low


def dot3(onehot, x):
    total = None
    for part in split3(x):
        term = jnp.dot(onehot, part, preferred_element_type=F32)
        total = term if total is None else total + term
    return total


def kernel(
    n_lat, n_lon,
    courant, obs, weight, innov, owner, row, count,
    inc_out, res_out,
    rate_in, rates, obs_v, terms, codes, code_out, spread_mat, gather_mat,
    field, moved, parts_t, parts_o, fetch_out, fetch_in, red_lon, red_lat,
    obs_sem, own_sem, wide_send, wide_recv, fetch_send, fetch_recv, part_send, part_recv,
    lon_send, lon_recv, lat_send, lat_recv,
):
    li = lax.axis_index("lat")
    lo = lax.axis_index("lon")
    levels, clat, clon = inc_out.shape
    cap = obs_v.shape[0]
    share = levels // n_lon
    ext = clat + 2 * HALO
    tile_rows = n_lon * ext
    n_src = 3 * n_lon

    obs_copy = pltpu.make_async_copy(obs.at[0], obs_v, obs_sem)
    obs_copy.start()

    def exists(d):
        return (li + d >= 0) & (li + d < n_lat)

    def guarded(d, run):
        if d == 0:
            run()
        else:
            pl.when(exists(d))(run)

    pairs = [(d, j) for d in (-1, 1, 0) for j in range(n_lon) if (d, j) != (0, 0)]

    def lon_at(j):
        return lax.rem(lo + j + n_lon, n_lon)

    barrier = pltpu.get_barrier_semaphore()

    def greet(lat, lon):
        pl.semaphore_signal(barrier, inc=1, device_id={"lat": lat, "lon": lon}, device_id_type=MESH)

    for d in (-1, 1):
        def hello(d=d):
            for j in range(1, n_lon):
                greet(li + d, lon_at(j))
        guarded(d, hello)
    for j in range(1, n_lon):
        greet(li, lon_at(j))

    @pl.loop(1, n_lat)
    def _(j):
        greet(lax.rem(li + j, n_lat), lo)

    sub = lax.broadcasted_iota(jnp.int32, (cap, clon), 0)
    live = count[0, 0]
    scal = []
    for b in range(cap):
        r = row[0, b]
        lev = lax.div(r, jnp.int32(clat))
        scal.append((r - lev * clat, (lev * n_lon + owner[0, b, 0]) * ext))
    for d in (-1, 0, 1):
        tile = jnp.full((cap, clon), -1, jnp.int32)
        for b in range(cap):
            lat_local = scal[b][0] + (HALO - clat * d)
            ok = (lat_local >= 0) & (lat_local < ext) & (b < live)
            tile = jnp.where(sub == b, jnp.where(ok, scal[b][1] + lat_local, -1), tile)
        code_out[d + 1] = tile.astype(F32)

    sides = (li > 0).astype(jnp.int32) + (li < n_lat - 1).astype(jnp.int32)
    pl.semaphore_wait(barrier, (n_lon - 1) + (n_lat - 1) + sides * (n_lon - 1))

    def wide(kind, d, j, src, dst):
        return pltpu.make_async_remote_copy(
            src_ref=src, dst_ref=dst,
            send_sem=wide_send.at[kind, d + 1, j], recv_sem=wide_recv.at[kind, d + 1, j],
            device_id={"lat": li + d, "lon": lon_at(j)}, device_id_type=MESH,
        )

    def send_slot(d):
        return (1 - d) * n_lon + lo

    def recv_slot(d, j):
        return (1 - d) * n_lon + lon_at(-j)

    def code_copy(d, j, slot):
        return wide(0, d, j, code_out.at[d + 1], codes.at[slot])

    def rate_copy(d, j, peer, tile):
        levs = pl.ds(peer * share, share)
        if d == 0:
            src, dst = pl.ds(0, clat), pl.ds(HALO, clat)
        elif d == 1:
            src, dst = pl.ds(clat - HALO, HALO), pl.ds(0, HALO)
        else:
            src, dst = pl.ds(0, HALO), pl.ds(HALO + clat, HALO)
        return wide(1, d, j, courant.at[:, levs, src, :], rate_in.at[:, :, tile, dst, :])

    def term_copy(rnd, d, j, slot):
        return wide(2 + rnd, d, j, terms.at[rnd, n_lon + lo], terms.at[rnd, slot])

    def start_wide(make):
        for d in (-1, 1, 0):
            def run(d=d):
                for j in range(n_lon):
                    if (d, j) != (0, 0):
                        make(d, j, True).start()
            guarded(d, run)

    def recv_wide(make):
        for d in (-1, 1, 0):
            def run(d=d):
                for j in range(n_lon):
                    if (d, j) != (0, 0):
                        make(d, j, False).wait_recv()
            guarded(-d, run)

    def done_wide(make):
        for d in (-1, 1, 0):
            def run(d=d):
                for j in range(n_lon):
                    if (d, j) != (0, 0):
                        make(d, j, True).wait_send()
            guarded(d, run)

    def code_make(d, j, out):
        return code_copy(d, j, send_slot(d) if out else recv_slot(d, j))

    def rate_make(d, j, out):
        return rate_copy(d, j, lon_at(j), lo if out else lon_at(-j))

    def term_make(rnd):
        return lambda d, j, out: term_copy(rnd, d, j, send_slot(d) if out else recv_slot(d, j))

    own_rate = pltpu.make_async_copy(
        courant.at[:, pl.ds(lo * share, share), :, :],
        rate_in.at[:, :, lo, pl.ds(HALO, clat), :], own_sem)
    start_wide(rate_make)
    start_wide(code_make)
    own_rate.start()
    codes[n_lon + lo] = code_out[1]

    pad = codes.shape[0] - n_src
    none = jnp.full((n_lon, cap, clon), -1.0, F32)
    if pad:
        codes[n_src:] = jnp.full((pad, cap, clon), -1.0, F32)
        for rnd in range(3):
            terms[rnd, n_src:] = jnp.zeros((pad, cap, clon), F32)
    for d in (-1, 1):
        @pl.when(jnp.logical_not(exists(d)))
        def _(d=d):
            first = (d + 1) * n_lon
            codes[first:first + n_lon] = none
            for rnd in range(3):
                terms[rnd, first:first + n_lon] = jnp.zeros((n_lon, cap, clon), F32)
            lat0 = 0 if d == -1 else HALO + clat
            rate_in[:, :, :, lat0:lat0 + HALO, :] = jnp.zeros((2, share, n_lon, HALO, clon), F32)

    live_rows = sub < live
    w_rows = jnp.where(live_rows, weight[0], 0.0)
    wy_rows = w_rows * innov[0]
    stacked = jnp.concatenate([w_rows, wy_rows, jnp.zeros((clon - 2 * cap, clon), F32)], axis=0)
    columns = jnp.transpose(stacked)
    w_col = [columns[:, b:b + 1] for b in range(cap)]

    def spread(rnd, u_cols):
        out = [jnp.sum(obs_v[b] * u_cols[b], axis=0, keepdims=True) for b in range(cap)]
        terms[rnd, n_lon + lo] = jnp.concatenate(out, axis=0)
        start_wide(term_make(rnd))

    obs_copy.wait()
    spread(0, [columns[:, cap + b:cap + b + 1] for b in range(cap)])

    base = (lo * (share * tile_rows)).astype(F32)
    recv_wide(code_make)
    n_blocks = codes.shape[0] * cap
    flat_codes = codes[...].reshape(n_blocks, clon) - base
    code_row = jnp.transpose(flat_codes)[0:1, :]
    for k in range(share):
        place = lax.broadcasted_iota(jnp.int32, (tile_rows, n_blocks), 0).astype(F32) + float(k * tile_rows)
        spread_mat[k * tile_rows:(k + 1) * tile_rows, :] = jnp.where(place == code_row, 1.0, 0.0).astype(BF16)
    centre = flat_codes[n_lon * cap:2 * n_lon * cap, :]
    for c in range(share * tile_rows // clon):
        lane_place = lax.broadcasted_iota(jnp.int32, centre.shape, 1).astype(F32) + float(c * clon)
        gather_mat[:, c * clon:(c + 1) * clon] = jnp.where(lane_place == centre, 1.0, 0.0).astype(BF16)

    recv_wide(rate_make)
    own_rate.wait()
    for k in range(share):
        c0 = rate_in[0, k].reshape(tile_rows, clon)
        c1 = rate_in[1, k].reshape(tile_rows, clon)
        a, b = jnp.maximum(c0, 0.0), jnp.maximum(-c0, 0.0)
        e, f = jnp.maximum(c1, 0.0), jnp.maximum(-c1, 0.0)
        rates[0, k], rates[1, k], rates[2, k], rates[3, k] = a, b, e, f
        rates[4, k] = 1.0 - a - b - e - f

    lane = lax.broadcasted_iota(jnp.int32, (tile_rows, clon), 1)
    lat_ids = lax.broadcasted_iota(jnp.int32, (ext, clon), 0) + (li * clat - HALO)
    inside = jnp.where((lat_ids >= 0) & (lat_ids < n_lat * clat), 1.0, 0.0)
    inside = jnp.concatenate([inside] * n_lon, axis=0)

    def lat_up(x):
        return pltpu.roll(x, tile_rows - 1, 0)

    def lat_down(x):
        return pltpu.roll(x, 1, 0)

    def lon_up(x):
        xs = pltpu.roll(x, clon - 1, 1)
        return jnp.where(lane == clon - 1, jnp.concatenate([xs[ext:], xs[:ext]], axis=0), xs)

    def lon_down(x):
        xs = pltpu.roll(x, 1, 1)
        return jnp.where(lane == 0, jnp.concatenate([xs[-ext:], xs[:-ext]], axis=0), xs)

    def apply_model(rnd, forward):
        flat = dot3(spread_mat[...], terms[rnd].reshape(n_blocks, clon))
        field[...] = flat.reshape(share, tile_rows, clon)

        @pl.loop(0, share)
        def _(k):
            y = field[k]
            for _ in range(STEPS):
                y = (rates[4, k] * y + lat_up(rates[0, k] * y) + lat_down(rates[1, k] * y)
                     + lon_up(rates[2, k] * y) + lon_down(rates[3, k] * y))
            for t in range(n_lon):
                parts_t[rnd, t, k] = y[t * ext + HALO:t * ext + HALO + clat]
            if forward:
                x = y * inside
                for _ in range(STEPS):
                    x = (rates[4, k] * x + rates[0, k] * lat_down(x) + rates[1, k] * lat_up(x)
                         + rates[2, k] * lon_down(x) + rates[3, k] * lon_up(x))
                moved[k] = x

    def part_make(rnd, j, out):
        place = lo if out else lon_at(-j)
        return pltpu.make_async_remote_copy(
            src_ref=parts_t.at[rnd, lon_at(j)],
            dst_ref=parts_o.at[rnd, pl.ds(place * share, share)],
            send_sem=part_send.at[rnd, j], recv_sem=part_recv.at[rnd, j],
            device_id={"lat": li, "lon": lon_at(j)}, device_id_type=MESH)

    def send_parts(rnd):
        for j in range(1, n_lon):
            part_make(rnd, j, True).start()
        parts_o[rnd, pl.ds(lo * share, share)] = parts_t[rnd, lo]

    def fetch_make(rnd, j, out):
        place = lo if out else lon_at(-j)
        return pltpu.make_async_remote_copy(
            src_ref=fetch_out.at[rnd, lon_at(j)], dst_ref=fetch_in.at[rnd, place],
            send_sem=fetch_send.at[rnd, j], recv_sem=fetch_recv.at[rnd, j],
            device_id={"lat": li, "lon": lon_at(j)}, device_id_type=MESH)

    def send_fetch(rnd):
        seen = dot3(gather_mat[...], moved[...].reshape(share * tile_rows, clon))
        fetch_out[rnd] = seen.reshape(n_lon, cap, clon)
        for j in range(1, n_lon):
            fetch_make(rnd, j, True).start()
        fetch_in[rnd, lo] = fetch_out[rnd, lo]

    def observe(rnd):
        for j in range(1, n_lon):
            fetch_make(rnd, j, False).wait_recv()
        seen = jnp.sum(fetch_in[rnd], axis=0)
        return [jnp.sum(obs_v[b] * seen[b:b + 1, :], axis=1, keepdims=True) for b in range(cap)]

    def red_lon_make(rnd, j, out):
        return pltpu.make_async_remote_copy(
            src_ref=red_lon.at[rnd, lo], dst_ref=red_lon.at[rnd, lo if out else lon_at(-j)],
            send_sem=lon_send.at[rnd, j], recv_sem=lon_recv.at[rnd, j],
            device_id={"lat": li, "lon": lon_at(j)}, device_id_type=MESH)

    def red_lat_make(rnd, j, out):
        place = li if out else lax.rem(li - j + n_lat, n_lat)
        return pltpu.make_async_remote_copy(
            src_ref=red_lat.at[rnd, li], dst_ref=red_lat.at[rnd, place],
            send_sem=lat_send.at[rnd, j], recv_sem=lat_recv.at[rnd, j],
            device_id={"lat": lax.rem(li + j, n_lat), "lon": lo}, device_id_type=MESH)

    sums_row = lax.broadcasted_iota(jnp.int32, (8, clon), 0)

    def reduce_start(rnd, values):
        tile = jnp.zeros((8, clon), F32)
        for n, value in enumerate(values):
            tile = jnp.where(sums_row == n, value, tile)
        red_lon[rnd, lo] = tile
        for j in range(1, n_lon):
            red_lon_make(rnd, j, True).start()

    def reduce_turn(rnd):
        for j in range(1, n_lon):
            red_lon_make(rnd, j, False).wait_recv()
        red_lat[rnd, li] = jnp.sum(red_lon[rnd], axis=0)

        @pl.loop(1, n_lat)
        def _(j):
            red_lat_make(rnd, j, True).start()

    def reduce_end(rnd):
        @pl.loop(1, n_lat)
        def _(j):
            red_lat_make(rnd, j, False).wait_recv()
        return jnp.sum(red_lat[rnd], axis=0)

    def total(x):
        return jnp.sum(jnp.sum(x, axis=0, keepdims=True), axis=1, keepdims=True)

    def squares(x):
        return total(jnp.sum((x * x).reshape(-1, 8, clon), axis=0))

    def column_total(cols):
        return jnp.sum(sum(cols), axis=0, keepdims=True)

    recv_wide(term_make(0))
    apply_model(0, True)
    send_fetch(0)
    send_parts(0)
    bb_part = squares(parts_t[0])
    p1 = observe(0)
    u1 = [w_col[b] * p1[b] for b in range(cap)]
    spread(1, u1)
    reduce_start(0, [bb_part, column_total([u1[b] * p1[b] for b in range(cap)])])
    reduce_turn(0)
    recv_wide(term_make(1))
    apply_model(1, True)
    send_fetch(1)
    send_parts(1)
    sums = reduce_end(0)
    bb, s1 = sums[0:1, 0:1], sums[1:2, 0:1]
    alpha1 = bb / (bb + s1)
    left1 = s1 / (bb + s1)
    rr_part = squares(left1 * parts_t[0] - alpha1 * parts_t[1])
    g1 = observe(1)
    pr = [left1 * p1[b] - alpha1 * g1[b] for b in range(cap)]
    ur = [w_col[b] * pr[b] for b in range(cap)]
    spread(2, ur)
    reduce_start(1, [rr_part, column_total([ur[b] * pr[b] for b in range(cap)]),
                     column_total([ur[b] * p1[b] for b in range(cap)])])
    reduce_turn(1)
    recv_wide(term_make(2))
    apply_model(2, False)
    send_parts(2)
    sums = reduce_end(1)
    rr, srr, sr1 = sums[0:1, 0:1], sums[1:2, 0:1], sums[2:3, 0:1]
    beta = rr / bb
    curve = rr + beta * beta * bb + (srr + 2.0 * beta * sr1 + beta * beta * s1)
    alpha2 = rr / curve
    for rnd in range(3):
        for j in range(1, n_lon):
            part_make(rnd, j, False).wait_recv()

    @pl.loop(0, levels)
    def _(k):
        b0, t1, tr = parts_o[0, k], parts_o[1, k], parts_o[2, k]
        r1 = left1 * b0 - alpha1 * t1
        inc_out[k] = alpha1 * b0 + alpha2 * (r1 + beta * b0)
        res_out[k] = r1 - alpha2 * (r1 + tr + beta * (b0 + t1))

    done_wide(rate_make)
    done_wide(code_make)
    for rnd in range(3):
        done_wide(term_make(rnd))
        for j in range(1, n_lon):
            part_make(rnd, j, True).wait_send()
    for rnd in range(2):
        for j in range(1, n_lon):
            fetch_make(rnd, j, True).wait_send()
            red_lon_make(rnd, j, True).wait_send()

        @pl.loop(1, n_lat)
        def _(j, rnd=rnd):
            red_lat_make(rnd, j, True).wait_send()


def shards(n_lat, n_lon, courant, obs_matrix, obs_weight, innovation, block_owner, block_row, block_count):
    _, levels, clat, clon = courant.shape
    cap = block_row.shape[1]
    share = levels // n_lon
    ext = clat + 2 * HALO
    tile_rows = n_lon * ext
    unit = clon // cap
    src_pad = -(-3 * n_lon // unit) * unit
    vmem = pl.BlockSpec(memory_space=pltpu.VMEM)
    smem = pl.BlockSpec(memory_space=pltpu.SMEM)
    hbm = pl.BlockSpec(memory_space=pl.ANY)
    dma = pltpu.SemaphoreType.DMA
    out = jax.ShapeDtypeStruct((levels, clat, clon), F32)
    return pl.pallas_call(
        functools.partial(kernel, n_lat, n_lon),
        out_shape=(out, out),
        in_specs=[hbm, hbm, vmem, vmem, smem, smem, smem],
        out_specs=(vmem, vmem),
        scratch_shapes=[
            pltpu.VMEM((2, share, n_lon, ext, clon), F32),
            pltpu.VMEM((5, share, tile_rows, clon), F32),
            pltpu.VMEM((cap, clon, clon), F32),
            pltpu.VMEM((3, src_pad, cap, clon), F32),
            pltpu.VMEM((src_pad, cap, clon), F32),
            pltpu.VMEM((3, cap, clon), F32),
            pltpu.VMEM((share * tile_rows, src_pad * cap), BF16),
            pltpu.VMEM((n_lon * cap, share * tile_rows), BF16),
            pltpu.VMEM((share, tile_rows, clon), F32),
            pltpu.VMEM((share, tile_rows, clon), F32),
            pltpu.VMEM((3, n_lon, share, clat, clon), F32),
            pltpu.VMEM((3, levels, clat, clon), F32),
            pltpu.VMEM((2, n_lon, cap, clon), F32),
            pltpu.VMEM((2, n_lon, cap, clon), F32),
            pltpu.VMEM((2, n_lon, 8, clon), F32),
            pltpu.VMEM((2, n_lat, 8, clon), F32),
            dma, dma,
            dma((5, 3, n_lon)), dma((5, 3, n_lon)),
            dma((2, n_lon)), dma((2, n_lon)),
            dma((3, n_lon)), dma((3, n_lon)),
            dma((2, n_lon)), dma((2, n_lon)),
            dma((2, n_lat)), dma((2, n_lat)),
        ],
        compiler_params=pltpu.CompilerParams(collective_id=0, has_side_effects=True),
    )(courant, obs_matrix, obs_weight, innovation, block_owner, block_row, block_count)


def solution(mesh):
    placed = (
        P(None, None, "lat", "lon"),
        P("lat", "lon", None, None),
        P("lat", "lon", None),
        P("lat", "lon", None),
        P("lat", "lon", None),
        P("lat", "lon"),
        P("lat", "lon"),
    )
    return jax.shard_map(
        functools.partial(shards, mesh.shape["lat"], mesh.shape["lon"]),
        mesh=mesh,
        in_specs=placed,
        out_specs=(P(None, "lat", "lon"), P(None, "lat", "lon")),
        check_vma=False,
    )
```

```python
import functools

import jax
import jax.numpy as jnp
from jax import lax
from jax.experimental import pallas as pl
from jax.experimental.pallas import tpu as pltpu
from jax.sharding import PartitionSpec as P

STEPS = 4
HALO = 2 * STEPS
MESH = pl.DeviceIdType.MESH
F32 = jnp.float32
BF16 = jnp.bfloat16


def split3(x):
    hi = x.astype(BF16)
    rest = x - hi.astype(F32)
    mid = rest.astype(BF16)
    low = (rest - mid.astype(F32)).astype(BF16)
    return hi, mid, low


def dot3(onehot, x):
    total = None
    for part in split3(x):
        term = jnp.dot(onehot, part, preferred_element_type=F32)
        total = term if total is None else total + term
    return total


def kernel(
    n_lat, n_lon,
    courant, obs, weight, innov, owner, row, count,
    parts_o, coef_out,
    flow, rate_in, rates, obs_v, terms, codes, code_out, spread_mat, gather_mat,
    field, moved, parts_t, fetch_out, fetch_in, red_lon, red_lat,
    obs_sem, own_sem, flow_sem, wide_send, wide_recv, fetch_send, fetch_recv, part_send, part_recv,
    lon_send, lon_recv, lat_send, lat_recv,
):
    li = lax.axis_index("lat")
    lo = lax.axis_index("lon")
    _, levels, clat, clon = parts_o.shape
    cap = obs_v.shape[0]
    share = levels // n_lon
    ext = clat + 2 * HALO
    tile_rows = n_lon * ext
    n_src = 3 * n_lon

    flow_copy = pltpu.make_async_copy(courant, flow, flow_sem)
    flow_copy.start()
    obs_copy = pltpu.make_async_copy(obs.at[0], obs_v, obs_sem)
    obs_copy.start()

    def exists(d):
        return (li + d >= 0) & (li + d < n_lat)

    def guarded(d, run):
        if d == 0:
            run()
        else:
            pl.when(exists(d))(run)

    def lon_at(j):
        return lax.rem(lo + j + n_lon, n_lon)

    barrier = pltpu.get_barrier_semaphore()

    def greet(lat, lon):
        pl.semaphore_signal(barrier, inc=1, device_id={"lat": lat, "lon": lon}, device_id_type=MESH)

    @pl.loop(1, n_lat)
    def _(j):
        greet(lax.rem(li + j, n_lat), lo)

    for d in (-1, 1):
        def hello(d=d):
            for j in range(1, n_lon):
                greet(li + d, lon_at(j))
        guarded(d, hello)
    for j in range(1, n_lon):
        greet(li, lon_at(j))

    sub = lax.broadcasted_iota(jnp.int32, (cap, clon), 0)
    live = count[0, 0]
    scal = []
    for b in range(cap):
        r = row[0, b]
        lev = lax.div(r, jnp.int32(clat))
        scal.append((r - lev * clat, (lev * n_lon + owner[0, b]) * ext))
    for d in (-1, 0, 1):
        tile = jnp.full((cap, clon), -1, jnp.int32)
        for b in range(cap):
            lat_local = scal[b][0] + (HALO - clat * d)
            ok = (lat_local >= 0) & (lat_local < ext) & (b < live)
            tile = jnp.where(sub == b, jnp.where(ok, scal[b][1] + lat_local, -1), tile)
        code_out[d + 1] = tile.astype(F32)

    sides = (li > 0).astype(jnp.int32) + (li < n_lat - 1).astype(jnp.int32)
    pl.semaphore_wait(barrier, (n_lon - 1) + (n_lat - 1) + sides * (n_lon - 1))

    def wide(kind, d, j, src, dst):
        return pltpu.make_async_remote_copy(
            src_ref=src, dst_ref=dst,
            send_sem=wide_send.at[kind, d + 1, j], recv_sem=wide_recv.at[kind, d + 1, j],
            device_id={"lat": li + d, "lon": lon_at(j)}, device_id_type=MESH,
        )

    def send_slot(d):
        return (1 - d) * n_lon + lo

    def recv_slot(d, j):
        return (1 - d) * n_lon + lon_at(-j)

    def code_copy(d, j, slot):
        return wide(0, d, j, code_out.at[d + 1], codes.at[slot])

    def rate_copy(d, j, peer, tile):
        levs = pl.ds(peer * share, share)
        if d == 0:
            src, dst = pl.ds(0, clat), pl.ds(HALO, clat)
        elif d == 1:
            src, dst = pl.ds(clat - HALO, HALO), pl.ds(0, HALO)
        else:
            src, dst = pl.ds(0, HALO), pl.ds(HALO + clat, HALO)
        return wide(1, d, j, flow.at[:, levs, src, :], rate_in.at[:, :, tile, dst, :])

    def term_copy(rnd, d, j, slot):
        return wide(2 + rnd, d, j, terms.at[rnd, n_lon + lo], terms.at[rnd, slot])

    def start_wide(make):
        for d in (-1, 1, 0):
            def run(d=d):
                for j in range(n_lon):
                    if (d, j) != (0, 0):
                        make(d, j, True).start()
            guarded(d, run)

    def recv_wide(make):
        for d in (-1, 1, 0):
            def run(d=d):
                for j in range(n_lon):
                    if (d, j) != (0, 0):
                        make(d, j, False).wait_recv()
            guarded(-d, run)

    def done_wide(make):
        for d in (-1, 1, 0):
            def run(d=d):
                for j in range(n_lon):
                    if (d, j) != (0, 0):
                        make(d, j, True).wait_send()
            guarded(d, run)

    def code_make(d, j, out):
        return code_copy(d, j, send_slot(d) if out else recv_slot(d, j))

    def rate_make(d, j, out):
        return rate_copy(d, j, lon_at(j), lo if out else lon_at(-j))

    def term_make(rnd):
        return lambda d, j, out: term_copy(rnd, d, j, send_slot(d) if out else recv_slot(d, j))

    own_rate = pltpu.make_async_copy(
        flow.at[:, pl.ds(lo * share, share), :, :],
        rate_in.at[:, :, lo, pl.ds(HALO, clat), :], own_sem)
    flow_copy.wait()
    start_wide(rate_make)
    start_wide(code_make)
    own_rate.start()
    codes[n_lon + lo] = code_out[1]

    pad = codes.shape[0] - n_src
    none = jnp.full((n_lon, cap, clon), -1.0, F32)
    if pad:
        codes[n_src:] = jnp.full((pad, cap, clon), -1.0, F32)
        for rnd in range(3):
            terms[rnd, n_src:] = jnp.zeros((pad, cap, clon), F32)
    for d in (-1, 1):
        @pl.when(jnp.logical_not(exists(d)))
        def _(d=d):
            first = (d + 1) * n_lon
            codes[first:first + n_lon] = none
            for rnd in range(3):
                terms[rnd, first:first + n_lon] = jnp.zeros((n_lon, cap, clon), F32)
            lat0 = 0 if d == -1 else HALO + clat
            rate_in[:, :, :, lat0:lat0 + HALO, :] = jnp.zeros((2, share, n_lon, HALO, clon), F32)

    live_rows = sub < live
    w_rows = jnp.where(live_rows, weight[0], 0.0)
    wy_rows = w_rows * innov[0]
    stacked = jnp.concatenate([w_rows, wy_rows, jnp.zeros((clon - 2 * cap, clon), F32)], axis=0)
    columns = jnp.transpose(stacked)
    w_col = [columns[:, b:b + 1] for b in range(cap)]

    def spread(rnd, u_cols):
        out = [jnp.sum(obs_v[b] * u_cols[b], axis=0, keepdims=True) for b in range(cap)]
        terms[rnd, n_lon + lo] = jnp.concatenate(out, axis=0)
        start_wide(term_make(rnd))

    obs_copy.wait()
    spread(0, [columns[:, cap + b:cap + b + 1] for b in range(cap)])

    base = (lo * (share * tile_rows)).astype(F32)
    recv_wide(code_make)
    n_blocks = codes.shape[0] * cap
    flat_codes = codes[...].reshape(n_blocks, clon) - base
    code_row = jnp.transpose(flat_codes)[0:1, :]
    for k in range(share):
        place = lax.broadcasted_iota(jnp.int32, (tile_rows, n_blocks), 0).astype(F32) + float(k * tile_rows)
        spread_mat[k * tile_rows:(k + 1) * tile_rows, :] = jnp.where(place == code_row, 1.0, 0.0).astype(BF16)
    centre = flat_codes[n_lon * cap:2 * n_lon * cap, :]
    for c in range(share * tile_rows // clon):
        lane_place = lax.broadcasted_iota(jnp.int32, centre.shape, 1).astype(F32) + float(c * clon)
        gather_mat[:, c * clon:(c + 1) * clon] = jnp.where(lane_place == centre, 1.0, 0.0).astype(BF16)

    recv_wide(rate_make)
    own_rate.wait()
    for k in range(share):
        c0 = rate_in[0, k].reshape(tile_rows, clon)
        c1 = rate_in[1, k].reshape(tile_rows, clon)
        a, b = jnp.maximum(c0, 0.0), jnp.maximum(-c0, 0.0)
        e, f = jnp.maximum(c1, 0.0), jnp.maximum(-c1, 0.0)
        rates[0, k], rates[1, k], rates[2, k], rates[3, k] = a, b, e, f
        rates[4, k] = 1.0 - a - b - e - f

    lane = lax.broadcasted_iota(jnp.int32, (tile_rows, clon), 1)
    lat_ids = lax.broadcasted_iota(jnp.int32, (ext, clon), 0) + (li * clat - HALO)
    inside = jnp.where((lat_ids >= 0) & (lat_ids < n_lat * clat), 1.0, 0.0)
    inside = jnp.concatenate([inside] * n_lon, axis=0)

    def lat_up(x):
        return pltpu.roll(x, tile_rows - 1, 0)

    def lat_down(x):
        return pltpu.roll(x, 1, 0)

    def lon_up(x):
        xs = pltpu.roll(x, clon - 1, 1)
        return jnp.where(lane == clon - 1, jnp.concatenate([xs[ext:], xs[:ext]], axis=0), xs)

    def lon_down(x):
        xs = pltpu.roll(x, 1, 1)
        return jnp.where(lane == 0, jnp.concatenate([xs[-ext:], xs[:-ext]], axis=0), xs)

    def apply_model(rnd, forward):
        flat = dot3(spread_mat[...], terms[rnd].reshape(n_blocks, clon))
        field[...] = flat.reshape(share, tile_rows, clon)

        @pl.loop(0, share, unroll=share)
        def _(k):
            y = field[k]
            for _ in range(STEPS):
                y = (rates[4, k] * y + lat_up(rates[0, k] * y) + lat_down(rates[1, k] * y)
                     + lon_up(rates[2, k] * y) + lon_down(rates[3, k] * y))
            for t in range(n_lon):
                parts_t[rnd, t, k] = y[t * ext + HALO:t * ext + HALO + clat]
            if forward:
                x = y * inside
                for _ in range(STEPS):
                    x = (rates[4, k] * x + rates[0, k] * lat_down(x) + rates[1, k] * lat_up(x)
                         + rates[2, k] * lon_down(x) + rates[3, k] * lon_up(x))
                moved[k] = x

    def part_make(rnd, j, out):
        place = lo if out else lon_at(-j)
        return pltpu.make_async_remote_copy(
            src_ref=parts_t.at[rnd, lon_at(j)],
            dst_ref=parts_o.at[rnd, pl.ds(place * share, share)],
            send_sem=part_send.at[rnd, j], recv_sem=part_recv.at[rnd, j],
            device_id={"lat": li, "lon": lon_at(j)}, device_id_type=MESH)

    def send_parts(rnd):
        for j in range(1, n_lon):
            part_make(rnd, j, True).start()
        parts_o[rnd, pl.ds(lo * share, share)] = parts_t[rnd, lo]

    def fetch_make(rnd, j, out):
        place = lo if out else lon_at(-j)
        return pltpu.make_async_remote_copy(
            src_ref=fetch_out.at[rnd, lon_at(j)], dst_ref=fetch_in.at[rnd, place],
            send_sem=fetch_send.at[rnd, j], recv_sem=fetch_recv.at[rnd, j],
            device_id={"lat": li, "lon": lon_at(j)}, device_id_type=MESH)

    def send_fetch(rnd):
        seen = dot3(gather_mat[...], moved[...].reshape(share * tile_rows, clon))
        fetch_out[rnd] = seen.reshape(n_lon, cap, clon)
        for j in range(1, n_lon):
            fetch_make(rnd, j, True).start()
        fetch_in[rnd, lo] = fetch_out[rnd, lo]

    def observe(rnd):
        for j in range(1, n_lon):
            fetch_make(rnd, j, False).wait_recv()
        seen = jnp.sum(fetch_in[rnd], axis=0)
        return [jnp.sum(obs_v[b] * seen[b:b + 1, :], axis=1, keepdims=True) for b in range(cap)]

    def red_lon_make(rnd, j, out):
        return pltpu.make_async_remote_copy(
            src_ref=red_lon.at[rnd, lo], dst_ref=red_lon.at[rnd, lo if out else lon_at(-j)],
            send_sem=lon_send.at[rnd, j], recv_sem=lon_recv.at[rnd, j],
            device_id={"lat": li, "lon": lon_at(j)}, device_id_type=MESH)

    def red_lat_make(rnd, j, out):
        place = li if out else lax.rem(li - j + n_lat, n_lat)
        return pltpu.make_async_remote_copy(
            src_ref=red_lat.at[rnd, li], dst_ref=red_lat.at[rnd, place],
            send_sem=lat_send.at[rnd, j], recv_sem=lat_recv.at[rnd, j],
            device_id={"lat": lax.rem(li + j, n_lat), "lon": lo}, device_id_type=MESH)

    sums_row = lax.broadcasted_iota(jnp.int32, (8, clon), 0)

    def reduce_start(rnd, values):
        tile = jnp.zeros((8, clon), F32)
        for n, value in enumerate(values):
            tile = jnp.where(sums_row == n, value, tile)
        red_lon[rnd, lo] = tile
        for j in range(1, n_lon):
            red_lon_make(rnd, j, True).start()

    def reduce_turn(rnd):
        for j in range(1, n_lon):
            red_lon_make(rnd, j, False).wait_recv()
        red_lat[rnd, li] = jnp.sum(red_lon[rnd], axis=0)

        @pl.loop(1, n_lat)
        def _(j):
            red_lat_make(rnd, j, True).start()

    def reduce_end(rnd):
        @pl.loop(1, n_lat)
        def _(j):
            red_lat_make(rnd, j, False).wait_recv()
        return jnp.sum(red_lat[rnd], axis=0)

    def total(x):
        return jnp.sum(jnp.sum(x, axis=0, keepdims=True), axis=1, keepdims=True)

    def squares(x):
        return total(jnp.sum((x * x).reshape(-1, 8, clon), axis=0))

    def column_total(cols):
        return jnp.sum(sum(cols), axis=0, keepdims=True)

    recv_wide(term_make(0))
    apply_model(0, True)
    send_fetch(0)
    send_parts(0)
    bb_part = squares(parts_t[0])
    p1 = observe(0)
    u1 = [w_col[b] * p1[b] for b in range(cap)]
    spread(1, u1)
    reduce_start(0, [bb_part, column_total([u1[b] * p1[b] for b in range(cap)])])
    reduce_turn(0)
    recv_wide(term_make(1))
    apply_model(1, True)
    send_fetch(1)
    send_parts(1)
    sums = reduce_end(0)
    bb, s1 = sums[0:1, 0:1], sums[1:2, 0:1]
    alpha1 = bb / (bb + s1)
    left1 = s1 / (bb + s1)
    rr_part = squares(left1 * parts_t[0] - alpha1 * parts_t[1])
    g1 = observe(1)
    pr = [left1 * p1[b] - alpha1 * g1[b] for b in range(cap)]
    ur = [w_col[b] * pr[b] for b in range(cap)]
    spread(2, ur)
    reduce_start(1, [rr_part, column_total([ur[b] * pr[b] for b in range(cap)]),
                     column_total([ur[b] * p1[b] for b in range(cap)])])
    reduce_turn(1)
    recv_wide(term_make(2))
    apply_model(2, False)
    send_parts(2)
    sums = reduce_end(1)
    rr, srr, sr1 = sums[0:1, 0:1], sums[1:2, 0:1], sums[2:3, 0:1]
    beta = rr / bb
    curve = rr + beta * beta * bb + (srr + 2.0 * beta * sr1 + beta * beta * s1)
    alpha2 = rr / curve
    for rnd in range(3):
        for j in range(1, n_lon):
            part_make(rnd, j, False).wait_recv()

    coef_row = sums_row
    tile = jnp.zeros((8, clon), F32)
    for n, value in enumerate((alpha1, left1, alpha2, beta)):
        tile = jnp.where(coef_row == n, value, tile)
    coef_out[...] = tile

    done_wide(rate_make)
    done_wide(code_make)
    for rnd in range(3):
        done_wide(term_make(rnd))
        for j in range(1, n_lon):
            part_make(rnd, j, True).wait_send()
    for rnd in range(2):
        for j in range(1, n_lon):
            fetch_make(rnd, j, True).wait_send()
            red_lon_make(rnd, j, True).wait_send()

        @pl.loop(1, n_lat)
        def _(j, rnd=rnd):
            red_lat_make(rnd, j, True).wait_send()


def shards(n_lat, n_lon, courant, obs_matrix, obs_weight, innovation, block_owner, block_row, block_count):
    _, levels, clat, clon = courant.shape
    cap = block_row.shape[1]
    share = levels // n_lon
    ext = clat + 2 * HALO
    tile_rows = n_lon * ext
    unit = clon // cap
    src_pad = -(-3 * n_lon // unit) * unit
    vmem = pl.BlockSpec(memory_space=pltpu.VMEM)
    smem = pl.BlockSpec(memory_space=pltpu.SMEM)
    hbm = pl.BlockSpec(memory_space=pl.ANY)
    dma = pltpu.SemaphoreType.DMA
    parts, coef = pl.pallas_call(
        functools.partial(kernel, n_lat, n_lon),
        out_shape=(
            jax.ShapeDtypeStruct((3, levels, clat, clon), F32),
            jax.ShapeDtypeStruct((8, clon), F32),
        ),
        in_specs=[hbm, hbm, vmem, vmem, smem, smem, smem],
        out_specs=(vmem, vmem),
        scratch_shapes=[
            pltpu.VMEM((2, levels, clat, clon), F32),
            pltpu.VMEM((2, share, n_lon, ext, clon), F32),
            pltpu.VMEM((5, share, tile_rows, clon), F32),
            pltpu.VMEM((cap, clon, clon), F32),
            pltpu.VMEM((3, src_pad, cap, clon), F32),
            pltpu.VMEM((src_pad, cap, clon), F32),
            pltpu.VMEM((3, cap, clon), F32),
            pltpu.VMEM((share * tile_rows, src_pad * cap), BF16),
            pltpu.VMEM((n_lon * cap, share * tile_rows), BF16),
            pltpu.VMEM((share, tile_rows, clon), F32),
            pltpu.VMEM((share, tile_rows, clon), F32),
            pltpu.VMEM((3, n_lon, share, clat, clon), F32),
            pltpu.VMEM((2, n_lon, cap, clon), F32),
            pltpu.VMEM((2, n_lon, cap, clon), F32),
            pltpu.VMEM((2, n_lon, 8, clon), F32),
            pltpu.VMEM((2, n_lat, 8, clon), F32),
            dma, dma, dma,
            dma((5, 3, n_lon)), dma((5, 3, n_lon)),
            dma((2, n_lon)), dma((2, n_lon)),
            dma((3, n_lon)), dma((3, n_lon)),
            dma((2, n_lon)), dma((2, n_lon)),
            dma((2, n_lat)), dma((2, n_lat)),
        ],
        compiler_params=pltpu.CompilerParams(collective_id=0, has_side_effects=True),
    )(courant, obs_matrix, obs_weight, innovation, block_owner[:, :, 0], block_row, block_count)
    alpha1, left1, alpha2, beta = (coef[n][None, None, :] for n in range(4))
    b0, t1, tr = parts[0], parts[1], parts[2]
    r1 = left1 * b0 - alpha1 * t1
    increment = alpha1 * b0 + alpha2 * (r1 + beta * b0)
    residual = r1 - alpha2 * (r1 + tr + beta * (b0 + t1))
    return increment, residual


def solution(mesh):
    placed = (
        P(None, None, "lat", "lon"),
        P("lat", "lon", None, None),
        P("lat", "lon", None),
        P("lat", "lon", None),
        P("lat", "lon", None),
        P("lat", "lon"),
        P("lat", "lon"),
    )
    return jax.shard_map(
        functools.partial(shards, mesh.shape["lat"], mesh.shape["lon"]),
        mesh=mesh,
        in_specs=placed,
        out_specs=(P(None, "lat", "lon"), P(None, "lat", "lon")),
        check_vma=False,
    )
```

```python
import functools

import jax
import jax.numpy as jnp
from jax import lax
from jax.experimental import pallas as pl
from jax.experimental.pallas import tpu as pltpu
from jax.sharding import PartitionSpec as P

STEPS = 4
HALO = 2 * STEPS
MESH = pl.DeviceIdType.MESH
F32 = jnp.float32
BF16 = jnp.bfloat16


def split3(x):
    hi = x.astype(BF16)
    rest = x - hi.astype(F32)
    mid = rest.astype(BF16)
    low = (rest - mid.astype(F32)).astype(BF16)
    return hi, mid, low


def dot3(onehot, x):
    total = None
    for part in split3(x):
        term = jnp.dot(onehot, part, preferred_element_type=F32)
        total = term if total is None else total + term
    return total


def kernel(
    n_lat, n_lon,
    courant, obs, weight_in, innov_in, owner_in, row_in, count_in,
    parts_o, alpha1_out, left1_out, alpha2_out, beta_out,
    flow, rate_in,
    rates, obs_v, terms, codes, code_out, spread_mat, gather_mat,
    field, moved, parts_t, fetch_out, fetch_in, red_lon, red_lat,
    obs_sem, own_sem, flow_sem, wide_send, wide_recv, fetch_send, fetch_recv, part_send, part_recv,
    lon_send, lon_recv, lat_send, lat_recv,
    weight, innov, owner, row, count, input_sems,
):
    li = lax.axis_index("lat")
    lo = lax.axis_index("lon")
    _, levels, clat, clon = parts_o.shape
    cap = obs_v.shape[0]
    share = levels // n_lon
    ext = clat + 2 * HALO
    tile_rows = n_lon * ext
    n_src = 3 * n_lon

    flow_copy = pltpu.make_async_copy(courant, flow, flow_sem)
    flow_copy.start()
    small = [
        pltpu.make_async_copy(src, dst, input_sems.at[n])
        for n, (src, dst) in enumerate((
            (owner_in, owner), (row_in, row), (count_in, count), (weight_in, weight), (innov_in, innov)))
    ]
    for copy in small:
        copy.start()
    obs_copy = pltpu.make_async_copy(obs.at[0], obs_v, obs_sem)
    obs_copy.start()

    def exists(d):
        return (li + d >= 0) & (li + d < n_lat)

    def guarded(d, run):
        if d == 0:
            run()
        else:
            pl.when(exists(d))(run)

    def lon_at(j):
        return lax.rem(lo + j + n_lon, n_lon)

    barrier = pltpu.get_barrier_semaphore()

    def greet(lat, lon):
        pl.semaphore_signal(barrier, inc=1, device_id={"lat": lat, "lon": lon}, device_id_type=MESH)

    @pl.loop(1, n_lat)
    def _(j):
        greet(lax.rem(li + j, n_lat), lo)

    for d in (-1, 1):
        def hello(d=d):
            for j in range(1, n_lon):
                greet(li + d, lon_at(j))
        guarded(d, hello)
    for j in range(1, n_lon):
        greet(li, lon_at(j))

    for copy in small:
        copy.wait()

    sub = lax.broadcasted_iota(jnp.int32, (cap, clon), 0)
    live = count[0, 0]
    scal = []
    for b in range(cap):
        r = row[0, b]
        lev = lax.div(r, jnp.int32(clat))
        scal.append((r - lev * clat, (lev * n_lon + owner[0, b]) * ext))
    for d in (-1, 0, 1):
        tile = jnp.full((cap, clon), -1, jnp.int32)
        for b in range(cap):
            lat_local = scal[b][0] + (HALO - clat * d)
            ok = (lat_local >= 0) & (lat_local < ext) & (b < live)
            tile = jnp.where(sub == b, jnp.where(ok, scal[b][1] + lat_local, -1), tile)
        code_out[d + 1] = tile.astype(F32)

    sides = (li > 0).astype(jnp.int32) + (li < n_lat - 1).astype(jnp.int32)
    pl.semaphore_wait(barrier, (n_lon - 1) + (n_lat - 1) + sides * (n_lon - 1))

    def wide(kind, d, j, src, dst):
        return pltpu.make_async_remote_copy(
            src_ref=src, dst_ref=dst,
            send_sem=wide_send.at[kind, d + 1, j], recv_sem=wide_recv.at[kind, d + 1, j],
            device_id={"lat": li + d, "lon": lon_at(j)}, device_id_type=MESH,
        )

    def send_slot(d):
        return (1 - d) * n_lon + lo

    def recv_slot(d, j):
        return (1 - d) * n_lon + lon_at(-j)

    def code_copy(d, j, slot):
        return wide(0, d, j, code_out.at[d + 1], codes.at[slot])

    def rate_copy(d, j, peer, tile):
        levs = pl.ds(peer * share, share)
        if d == 0:
            src, dst = pl.ds(0, clat), pl.ds(HALO, clat)
        elif d == 1:
            src, dst = pl.ds(clat - HALO, HALO), pl.ds(0, HALO)
        else:
            src, dst = pl.ds(0, HALO), pl.ds(HALO + clat, HALO)
        return wide(1, d, j, flow.at[:, levs, src, :], rate_in.at[:, :, tile, dst, :])

    def term_copy(rnd, d, j, slot):
        return wide(2 + rnd, d, j, terms.at[rnd, n_lon + lo], terms.at[rnd, slot])

    def start_wide(make):
        for d in (-1, 1, 0):
            def run(d=d):
                for j in range(n_lon):
                    if (d, j) != (0, 0):
                        make(d, j, True).start()
            guarded(d, run)

    def recv_wide(make):
        for d in (-1, 1, 0):
            def run(d=d):
                for j in range(n_lon):
                    if (d, j) != (0, 0):
                        make(d, j, False).wait_recv()
            guarded(-d, run)

    def done_wide(make):
        for d in (-1, 1, 0):
            def run(d=d):
                for j in range(n_lon):
                    if (d, j) != (0, 0):
                        make(d, j, True).wait_send()
            guarded(d, run)

    def code_make(d, j, out):
        return code_copy(d, j, send_slot(d) if out else recv_slot(d, j))

    def rate_make(d, j, out):
        return rate_copy(d, j, lon_at(j), lo if out else lon_at(-j))

    def term_make(rnd):
        return lambda d, j, out: term_copy(rnd, d, j, send_slot(d) if out else recv_slot(d, j))

    own_rate = pltpu.make_async_copy(
        flow.at[:, pl.ds(lo * share, share), :, :],
        rate_in.at[:, :, lo, pl.ds(HALO, clat), :], own_sem)
    flow_copy.wait()
    start_wide(rate_make)
    start_wide(code_make)
    own_rate.start()
    codes[n_lon + lo] = code_out[1]

    pad = codes.shape[0] - n_src
    none = jnp.full((n_lon, cap, clon), -1.0, F32)
    if pad:
        codes[n_src:] = jnp.full((pad, cap, clon), -1.0, F32)
        for rnd in range(3):
            terms[rnd, n_src:] = jnp.zeros((pad, cap, clon), F32)
    for d in (-1, 1):
        @pl.when(jnp.logical_not(exists(d)))
        def _(d=d):
            first = (d + 1) * n_lon
            codes[first:first + n_lon] = none
            for rnd in range(3):
                terms[rnd, first:first + n_lon] = jnp.zeros((n_lon, cap, clon), F32)
            lat0 = 0 if d == -1 else HALO + clat
            rate_in[:, :, :, lat0:lat0 + HALO, :] = jnp.zeros((2, share, n_lon, HALO, clon), F32)

    live_rows = sub < live
    w_rows = jnp.where(live_rows, weight[0], 0.0)
    wy_rows = w_rows * innov[0]
    stacked = jnp.concatenate([w_rows, wy_rows, jnp.zeros((clon - 2 * cap, clon), F32)], axis=0)
    columns = jnp.transpose(stacked)
    w_col = [columns[:, b:b + 1] for b in range(cap)]

    def spread(rnd, u_cols):
        out = [jnp.sum(obs_v[b] * u_cols[b], axis=0, keepdims=True) for b in range(cap)]
        terms[rnd, n_lon + lo] = jnp.concatenate(out, axis=0)
        start_wide(term_make(rnd))

    obs_copy.wait()
    spread(0, [columns[:, cap + b:cap + b + 1] for b in range(cap)])

    base = (lo * (share * tile_rows)).astype(F32)
    recv_wide(code_make)
    n_blocks = codes.shape[0] * cap
    flat_codes = codes[...].reshape(n_blocks, clon) - base
    code_row = jnp.transpose(flat_codes)[0:1, :]
    for k in range(share):
        place = lax.broadcasted_iota(jnp.int32, (tile_rows, n_blocks), 0).astype(F32) + float(k * tile_rows)
        spread_mat[k * tile_rows:(k + 1) * tile_rows, :] = jnp.where(place == code_row, 1.0, 0.0).astype(BF16)
    centre = flat_codes[n_lon * cap:2 * n_lon * cap, :]
    for c in range(share * tile_rows // clon):
        lane_place = lax.broadcasted_iota(jnp.int32, centre.shape, 1).astype(F32) + float(c * clon)
        gather_mat[:, c * clon:(c + 1) * clon] = jnp.where(lane_place == centre, 1.0, 0.0).astype(BF16)

    recv_wide(rate_make)
    own_rate.wait()
    for k in range(share):
        c0 = rate_in[0, k].reshape(tile_rows, clon)
        c1 = rate_in[1, k].reshape(tile_rows, clon)
        a, b = jnp.maximum(c0, 0.0), jnp.maximum(-c0, 0.0)
        e, f = jnp.maximum(c1, 0.0), jnp.maximum(-c1, 0.0)
        rates[0, k], rates[1, k], rates[2, k], rates[3, k] = a, b, e, f
        rates[4, k] = 1.0 - a - b - e - f

    lane = lax.broadcasted_iota(jnp.int32, (tile_rows, clon), 1)
    lat_ids = lax.broadcasted_iota(jnp.int32, (ext, clon), 0) + (li * clat - HALO)
    inside = jnp.where((lat_ids >= 0) & (lat_ids < n_lat * clat), 1.0, 0.0)
    inside = jnp.concatenate([inside] * n_lon, axis=0)

    def lat_up(x):
        return pltpu.roll(x, tile_rows - 1, 0)

    def lat_down(x):
        return pltpu.roll(x, 1, 0)

    def lon_up(x):
        xs = pltpu.roll(x, clon - 1, 1)
        return jnp.where(lane == clon - 1, jnp.concatenate([xs[ext:], xs[:ext]], axis=0), xs)

    def lon_down(x):
        xs = pltpu.roll(x, 1, 1)
        return jnp.where(lane == 0, jnp.concatenate([xs[-ext:], xs[:-ext]], axis=0), xs)

    def apply_model(rnd, forward):
        flat = dot3(spread_mat[...], terms[rnd].reshape(n_blocks, clon))
        field[...] = flat.reshape(share, tile_rows, clon)

        @pl.loop(0, share, unroll=share)
        def _(k):
            y = field[k]
            for _ in range(STEPS):
                y = (rates[4, k] * y + lat_up(rates[0, k] * y) + lat_down(rates[1, k] * y)
                     + lon_up(rates[2, k] * y) + lon_down(rates[3, k] * y))
            for t in range(n_lon):
                parts_t[rnd, t, k] = y[t * ext + HALO:t * ext + HALO + clat]
            if forward:
                x = y * inside
                for _ in range(STEPS):
                    x = (rates[4, k] * x + rates[0, k] * lat_down(x) + rates[1, k] * lat_up(x)
                         + rates[2, k] * lon_down(x) + rates[3, k] * lon_up(x))
                moved[k] = x

    def part_make(rnd, j, out):
        place = lo if out else lon_at(-j)
        return pltpu.make_async_remote_copy(
            src_ref=parts_t.at[rnd, lon_at(j)],
            dst_ref=parts_o.at[rnd, pl.ds(place * share, share)],
            send_sem=part_send.at[rnd, j], recv_sem=part_recv.at[rnd, j],
            device_id={"lat": li, "lon": lon_at(j)}, device_id_type=MESH)

    def send_parts(rnd):
        for j in range(1, n_lon):
            part_make(rnd, j, True).start()
        parts_o[rnd, pl.ds(lo * share, share)] = parts_t[rnd, lo]

    def fetch_make(rnd, j, out):
        place = lo if out else lon_at(-j)
        return pltpu.make_async_remote_copy(
            src_ref=fetch_out.at[rnd, lon_at(j)], dst_ref=fetch_in.at[rnd, place],
            send_sem=fetch_send.at[rnd, j], recv_sem=fetch_recv.at[rnd, j],
            device_id={"lat": li, "lon": lon_at(j)}, device_id_type=MESH)

    def send_fetch(rnd):
        seen = dot3(gather_mat[...], moved[...].reshape(share * tile_rows, clon))
        fetch_out[rnd] = seen.reshape(n_lon, cap, clon)
        for j in range(1, n_lon):
            fetch_make(rnd, j, True).start()
        fetch_in[rnd, lo] = fetch_out[rnd, lo]

    def observe(rnd):
        for j in range(1, n_lon):
            fetch_make(rnd, j, False).wait_recv()
        seen = jnp.sum(fetch_in[rnd], axis=0)
        return [jnp.sum(obs_v[b] * seen[b:b + 1, :], axis=1, keepdims=True) for b in range(cap)]

    def red_lon_make(rnd, j, out):
        return pltpu.make_async_remote_copy(
            src_ref=red_lon.at[rnd, lo], dst_ref=red_lon.at[rnd, lo if out else lon_at(-j)],
            send_sem=lon_send.at[rnd, j], recv_sem=lon_recv.at[rnd, j],
            device_id={"lat": li, "lon": lon_at(j)}, device_id_type=MESH)

    def red_lat_make(rnd, j, out):
        place = li if out else lax.rem(li - j + n_lat, n_lat)
        return pltpu.make_async_remote_copy(
            src_ref=red_lat.at[rnd, li], dst_ref=red_lat.at[rnd, place],
            send_sem=lat_send.at[rnd, j], recv_sem=lat_recv.at[rnd, j],
            device_id={"lat": lax.rem(li + j, n_lat), "lon": lo}, device_id_type=MESH)

    sums_row = lax.broadcasted_iota(jnp.int32, (8, clon), 0)

    def reduce_start(rnd, values):
        tile = jnp.zeros((8, clon), F32)
        for n, value in enumerate(values):
            tile = jnp.where(sums_row == n, value, tile)
        red_lon[rnd, lo] = tile
        for j in range(1, n_lon):
            red_lon_make(rnd, j, True).start()

    def reduce_turn(rnd):
        for j in range(1, n_lon):
            red_lon_make(rnd, j, False).wait_recv()
        red_lat[rnd, li] = jnp.sum(red_lon[rnd], axis=0)

        @pl.loop(1, n_lat)
        def _(j):
            red_lat_make(rnd, j, True).start()

    def reduce_end(rnd):
        @pl.loop(1, n_lat)
        def _(j):
            red_lat_make(rnd, j, False).wait_recv()
        return jnp.sum(red_lat[rnd], axis=0)

    def total(x):
        return jnp.sum(jnp.sum(x, axis=0, keepdims=True), axis=1, keepdims=True)

    def squares(x):
        return total(jnp.sum((x * x).reshape(-1, 8, clon), axis=0))

    def column_total(cols):
        return jnp.sum(sum(cols), axis=0, keepdims=True)

    recv_wide(term_make(0))
    apply_model(0, True)
    send_fetch(0)
    send_parts(0)
    bb_part = squares(parts_t[0])
    p1 = observe(0)
    u1 = [w_col[b] * p1[b] for b in range(cap)]
    spread(1, u1)
    reduce_start(0, [bb_part, column_total([u1[b] * p1[b] for b in range(cap)])])
    reduce_turn(0)
    recv_wide(term_make(1))
    apply_model(1, True)
    send_fetch(1)
    send_parts(1)
    sums = reduce_end(0)
    bb, s1 = sums[0:1, 0:1], sums[1:2, 0:1]
    alpha1 = bb / (bb + s1)
    left1 = s1 / (bb + s1)
    rr_part = squares(left1 * parts_t[0] - alpha1 * parts_t[1])
    g1 = observe(1)
    pr = [left1 * p1[b] - alpha1 * g1[b] for b in range(cap)]
    ur = [w_col[b] * pr[b] for b in range(cap)]
    spread(2, ur)
    reduce_start(1, [rr_part, column_total([ur[b] * pr[b] for b in range(cap)]),
                     column_total([ur[b] * p1[b] for b in range(cap)])])
    reduce_turn(1)
    recv_wide(term_make(2))
    apply_model(2, False)
    send_parts(2)
    sums = reduce_end(1)
    rr, srr, sr1 = sums[0:1, 0:1], sums[1:2, 0:1], sums[2:3, 0:1]
    beta = rr / bb
    curve = rr + beta * beta * bb + (srr + 2.0 * beta * sr1 + beta * beta * s1)
    alpha2 = rr / curve
    for rnd in range(3):
        for j in range(1, n_lon):
            part_make(rnd, j, False).wait_recv()

    for ref, value in ((alpha1_out, alpha1), (left1_out, left1), (alpha2_out, alpha2), (beta_out, beta)):
        ref[...] = jnp.broadcast_to(value, (1, clon)).reshape(1, 1, clon)

    done_wide(rate_make)
    done_wide(code_make)
    for rnd in range(3):
        done_wide(term_make(rnd))
        for j in range(1, n_lon):
            part_make(rnd, j, True).wait_send()
    for rnd in range(2):
        for j in range(1, n_lon):
            fetch_make(rnd, j, True).wait_send()
            red_lon_make(rnd, j, True).wait_send()

        @pl.loop(1, n_lat)
        def _(j, rnd=rnd):
            red_lat_make(rnd, j, True).wait_send()


def shards(n_lat, n_lon, courant, obs_matrix, obs_weight, innovation, block_owner, block_row, block_count):
    _, levels, clat, clon = courant.shape
    cap = block_row.shape[1]
    share = levels // n_lon
    ext = clat + 2 * HALO
    tile_rows = n_lon * ext
    unit = clon // cap
    src_pad = -(-3 * n_lon // unit) * unit
    vmem = pl.BlockSpec(memory_space=pltpu.VMEM)
    hbm = pl.BlockSpec(memory_space=pl.ANY)
    dma = pltpu.SemaphoreType.DMA
    scalar = jax.ShapeDtypeStruct((1, 1, clon), F32)
    parts, alpha1, left1, alpha2, beta = pl.pallas_call(
        functools.partial(kernel, n_lat, n_lon),
        out_shape=(
            jax.ShapeDtypeStruct((3, levels, clat, clon), F32),
            scalar, scalar, scalar, scalar,
        ),
        in_specs=[hbm] * 7,
        out_specs=(vmem,) * 5,
        scratch_shapes=[
            pltpu.VMEM((2, levels, clat, clon), F32),
            pltpu.VMEM((2, share, n_lon, ext, clon), F32),
            pltpu.VMEM((5, share, tile_rows, clon), F32),
            pltpu.VMEM((cap, clon, clon), F32),
            pltpu.VMEM((3, src_pad, cap, clon), F32),
            pltpu.VMEM((src_pad, cap, clon), F32),
            pltpu.VMEM((3, cap, clon), F32),
            pltpu.VMEM((share * tile_rows, src_pad * cap), BF16),
            pltpu.VMEM((n_lon * cap, share * tile_rows), BF16),
            pltpu.VMEM((share, tile_rows, clon), F32),
            pltpu.VMEM((share, tile_rows, clon), F32),
            pltpu.VMEM((3, n_lon, share, clat, clon), F32),
            pltpu.VMEM((2, n_lon, cap, clon), F32),
            pltpu.VMEM((2, n_lon, cap, clon), F32),
            pltpu.VMEM((2, n_lon, 8, clon), F32),
            pltpu.VMEM((2, n_lat, 8, clon), F32),
            dma, dma, dma,
            dma((5, 3, n_lon)), dma((5, 3, n_lon)),
            dma((2, n_lon)), dma((2, n_lon)),
            dma((3, n_lon)), dma((3, n_lon)),
            dma((2, n_lon)), dma((2, n_lon)),
            dma((2, n_lat)), dma((2, n_lat)),
            pltpu.VMEM((1, cap, clon), F32), pltpu.VMEM((1, cap, clon), F32),
            pltpu.SMEM((1, cap), jnp.int32), pltpu.SMEM((1, cap), jnp.int32),
            pltpu.SMEM((1, 1), jnp.int32),
            dma((5,)),
        ],
        compiler_params=pltpu.CompilerParams(collective_id=0, has_side_effects=True),
    )(courant, obs_matrix, obs_weight, innovation, block_owner[:, :, 0], block_row, block_count)
    b0, t1, tr = parts[0], parts[1], parts[2]
    r1 = left1 * b0 - alpha1 * t1
    increment = alpha1 * b0 + alpha2 * (r1 + beta * b0)
    residual = r1 - alpha2 * (r1 + tr + beta * (b0 + t1))
    return increment, residual


def solution(mesh):
    placed = (
        P(None, None, "lat", "lon"),
        P("lat", "lon", None, None),
        P("lat", "lon", None),
        P("lat", "lon", None),
        P("lat", "lon", None),
        P("lat", "lon"),
        P("lat", "lon"),
    )
    return jax.shard_map(
        functools.partial(shards, mesh.shape["lat"], mesh.shape["lon"]),
        mesh=mesh,
        in_specs=placed,
        out_specs=(P(None, "lat", "lon"), P(None, "lat", "lon")),
        check_vma=False,
    )
```
